32 devices in a mesh: rep: 1 (over z), ep: 4 (over y), fsdp: 8 (over x, core).
Axes of the slice: x: 4, y: 4, z: 1, core: 2. Of those that a mesh axis runs over, the one named last changes fastest.
The devices are a block of a 4x4x8 slice.
Arguments:
- x: bfloat16 [32768, 1024], P(('rep', 'ep', 'fsdp'))
- norm_w: float32 [2, 1024], replicated
- router_w: bfloat16 [2, 1024, 32], replicated
- w_gate: bfloat16 [2, 32, 1024, 512], P(None, 'ep', None, 'fsdp')
- w_up: bfloat16 [2, 32, 1024, 512], P(None, 'ep', None, 'fsdp')
- w_down: bfloat16 [2, 32, 512, 1024], P(None, 'ep', 'fsdp')
- expert_idx: int32 [2, 32768, 8], P(None, ('rep', 'ep', 'fsdp'))
Outputs:
- output: bfloat16 [32768, 1024], P(('rep', 'ep', 'fsdp'))
All inputs are finite; a program needn't handle non-finite values.
Results may differ from the reference program's by a relative error of at most 0.012267.
Values are sent between devices in bfloat16 or wider.
A program may use at most 768 MiB of HBM per device.

```python
import jax
import jax.numpy as jnp
from jax import lax

MODEL_DIM = 1024
FFN_DIM = 512
EXPERTS = 32
TOP_K = 8
LAYERS = 2
TOKENS = 32768
NORM_EPS = 1e-5
ROW_BLOCK = min(TOKENS, 1024)


def draw_routing(key):
    key_noise, key_hot = jax.random.split(key)
    noise_int = jax.random.randint(key_noise, (LAYERS, TOKENS, EXPERTS), 0, 4096)
    hot_bias = jax.random.randint(key_hot, (LAYERS, 1, EXPERTS), 0, 3072)
    expert_ids = jnp.arange(EXPERTS, dtype=jnp.int32)
    cover_bonus = jnp.where((jnp.arange(TOKENS, dtype=jnp.int32) % EXPERTS)[:, None] == expert_ids[None, :], 16384, 0)
    score_int = (noise_int + hot_bias + cover_bonus[None]) * EXPERTS + expert_ids
    return lax.top_k(score_int, TOP_K)[1].astype(jnp.int32)


def setup_inputs(seed: int = 0, part: int = 0) -> dict:
    shared = jax.random.key(seed)
    part_key = jax.random.fold_in(shared, part)
    key_x, key_route = jax.random.split(part_key)
    key_list = jax.random.split(shared, 5)
    x = jax.random.normal(key_x, (TOKENS, MODEL_DIM), jnp.float32).astype(jnp.bfloat16)
    norm_w = 1.0 + 0.5 * jax.random.uniform(key_list[0], (LAYERS, MODEL_DIM), jnp.float32, -1.0, 1.0)
    router_w = (2.0 * MODEL_DIM ** -0.5 * jax.random.normal(key_list[1], (LAYERS, MODEL_DIM, EXPERTS), jnp.float32)).astype(jnp.bfloat16)
    w_gate = (MODEL_DIM ** -0.5 * jax.random.normal(key_list[2], (LAYERS, EXPERTS, MODEL_DIM, FFN_DIM), jnp.float32)).astype(jnp.bfloat16)
    w_up = (MODEL_DIM ** -0.5 * jax.random.normal(key_list[3], (LAYERS, EXPERTS, MODEL_DIM, FFN_DIM), jnp.float32)).astype(jnp.bfloat16)
    w_down = (2.0 * FFN_DIM ** -0.5 * jax.random.normal(key_list[4], (LAYERS, EXPERTS, FFN_DIM, MODEL_DIM), jnp.float32)).astype(jnp.bfloat16)
    expert_idx = draw_routing(key_route)
    return {"x": x, "norm_w": norm_w, "router_w": router_w, "w_gate": w_gate, "w_up": w_up, "w_down": w_down, "expert_idx": expert_idx}


def moe_block(x_blk, idx_blk, norm_w, router_w, w_gate, w_up, w_down):
    x_f32 = x_blk.astype(jnp.float32)
    normed = (x_f32 * lax.rsqrt(jnp.mean(x_f32 * x_f32, axis=-1, keepdims=True) + NORM_EPS) * norm_w).astype(jnp.bfloat16)
    logits = jnp.dot(normed, router_w, preferred_element_type=jnp.float32)
    gate_wts = jax.nn.softmax(jnp.take_along_axis(logits, idx_blk, axis=1), axis=-1)
    expert_ids = jnp.arange(EXPERTS, dtype=jnp.int32)
    coeff_te = jnp.sum(jnp.where(idx_blk[:, :, None] == expert_ids[None, None, :], gate_wts[:, :, None], 0.0), axis=1)

    def expert_step(acc_out, packed):
        gate_e, up_e, down_e, coeff_e = packed
        gate_proj = jnp.dot(normed, gate_e, preferred_element_type=jnp.float32)
        up_proj = jnp.dot(normed, up_e, preferred_element_type=jnp.float32)
        hidden_act = (jax.nn.silu(gate_proj) * up_proj).astype(jnp.bfloat16)
        expert_out = jnp.dot(hidden_act, down_e, preferred_element_type=jnp.float32)
        return acc_out + coeff_e[:, None] * expert_out, None

    init_acc = jnp.zeros((ROW_BLOCK, MODEL_DIM), jnp.float32)
    mixed = lax.scan(expert_step, init_acc, (w_gate, w_up, w_down, coeff_te.T))[0]
    return (x_f32 + mixed).astype(jnp.bfloat16)


def reference(x, norm_w, router_w, w_gate, w_up, w_down, expert_idx):
    blocks = TOKENS // ROW_BLOCK

    def layer_step(x_cur, layer_args):
        norm_l, router_l, gate_l, up_l, down_l, idx_l = layer_args

        def block_fn(packed):
            return moe_block(packed[0], packed[1], norm_l, router_l, gate_l, up_l, down_l)

        new_rows = lax.map(block_fn, (x_cur.reshape(blocks, ROW_BLOCK, MODEL_DIM), idx_l.reshape(blocks, ROW_BLOCK, TOP_K)))
        return new_rows.reshape(TOKENS, MODEL_DIM), None

    return lax.scan(layer_step, x, (norm_w, router_w, w_gate, w_up, w_down, expert_idx))[0]
```

```python
import jax
import jax.numpy as jnp
from jax import lax
from jax.experimental import pallas as pl
from jax.experimental.pallas import tpu as pltpu
from jax.sharding import PartitionSpec as P

NORM_EPS = 1e-5
NT = (((1,), (1,)), ((), ()))


def rms_norm(x, norm_w):
    x_f32 = x.astype(jnp.float32)
    return (x_f32 * lax.rsqrt(jnp.mean(x_f32 * x_f32, axis=-1, keepdims=True) + NORM_EPS) * norm_w).astype(jnp.bfloat16)


def route_coeffs(normed, router_w, expert_idx):
    experts = router_w.shape[-1]
    logits = jnp.dot(normed, router_w, preferred_element_type=jnp.float32)
    hit = jnp.any(expert_idx[:, :, None] == jnp.arange(experts, dtype=jnp.int32), axis=1)
    top = jnp.max(jnp.where(hit, logits, -jnp.inf), axis=-1, keepdims=True)
    exps = jnp.where(hit, jnp.exp(jnp.where(hit, logits - top, 0.0)), 0.0)
    return exps / jnp.sum(exps, axis=-1, keepdims=True)


def expert_ffn(h_ref, coeff, wg_ref, wu_ref, wd_ref, act_ref, acc_ref, first):
    width, dim = wd_ref.shape
    fc, nc = min(width, 256), min(dim, 256)
    for f in range(width // fc):
        rows = pl.ds(f * fc, fc)
        u = lax.dot_general(h_ref[...], wg_ref[rows, :], NT, preferred_element_type=jnp.float32)
        v = lax.dot_general(h_ref[...], wu_ref[rows, :], NT, preferred_element_type=jnp.float32)
        act_ref[:, rows] = (jax.nn.silu(u) * v).astype(jnp.bfloat16)
    for n in range(dim // nc):
        cols = pl.ds(n * nc, nc)
        o = coeff * jnp.dot(act_ref[...], wd_ref[:, cols], preferred_element_type=jnp.float32)
        acc_ref[:, cols] = jnp.where(first, 0.0, acc_ref[:, cols]) + o


def ffn_kernel(h_ref, c_ref, w_ref, out_ref, w_flat, act_ref):
    e = pl.program_id(1)
    pieces, _, _, rows, dim = w_ref.shape
    lane = lax.broadcasted_iota(jnp.int32, c_ref.shape, 1)
    coeff = jnp.sum(jnp.where(lane == e, c_ref[...], 0.0), axis=1, keepdims=True)
    for m in range(3):
        w_flat[m] = w_ref[:, 0, m].reshape(pieces * rows, dim)
    expert_ffn(h_ref, coeff, w_flat.at[0], w_flat.at[1], w_flat.at[2], act_ref, out_ref, e == 0)


def dense_ffn(h, coeff, w):
    tokens, dim = h.shape
    pieces, experts, _, rows, _ = w.shape
    tb = min(tokens, 1024)
    return pl.pallas_call(
        ffn_kernel,
        grid=(tokens // tb, experts),
        in_specs=[
            pl.BlockSpec((tb, dim), lambda t, e: (t, 0)),
            pl.BlockSpec((tb, experts), lambda t, e: (t, 0)),
            pl.BlockSpec((pieces, 1, 3, rows, dim), lambda t, e: (0, e, 0, 0, 0)),
        ],
        out_specs=pl.BlockSpec((tb, dim), lambda t, e: (t, 0)),
        out_shape=jax.ShapeDtypeStruct((tokens, dim), jnp.float32),
        scratch_shapes=[pltpu.VMEM((3, pieces * rows, dim), jnp.bfloat16), pltpu.VMEM((tb, pieces * rows), jnp.bfloat16)],
        compiler_params=pltpu.CompilerParams(dimension_semantics=("arbitrary", "arbitrary"), vmem_limit_bytes=60 << 20),
        cost_estimate=pl.CostEstimate(
            flops=6 * tokens * experts * pieces * rows * dim, bytes_accessed=w.size * 2 * (tokens // tb), transcendentals=0
        ),
    )(h, coeff, w)


def solution(mesh):
    tok_spec = P(("rep", "ep", "fsdp"), None)
    idx_spec = P(None, ("rep", "ep", "fsdp"), None)
    in_specs = (tok_spec, P(None, None), P(None, None, None), P(None, "ep", None, "fsdp"), P(None, "ep", None, "fsdp"), P(None, "ep", "fsdp", None), idx_spec)

    def local_program(x, norm_w, router_w, w_gate, w_up, w_down, expert_idx):
        layers, experts = w_gate.shape[:2]
        packed = jnp.stack([w_gate.transpose(0, 1, 3, 2), w_up.transpose(0, 1, 3, 2), w_down], axis=2)
        gathered = [lax.all_gather(packed[l], "fsdp", axis=0) for l in range(layers)]
        for l in range(layers):
            normed = rms_norm(x, norm_w[l])
            coeff = route_coeffs(normed, router_w[l], expert_idx[l])
            h_all = lax.all_gather(normed, "ep", axis=0, tiled=True)
            c_all = lax.all_gather(coeff, "ep", axis=0, tiled=True)
            c_own = lax.dynamic_slice_in_dim(c_all, lax.axis_index("ep") * experts, experts, axis=1)
            partial = dense_ffn(h_all, c_own, gathered[l])
            mixed = lax.psum_scatter(partial, "ep", scatter_dimension=0, tiled=True)
            x = (x.astype(jnp.float32) + mixed).astype(jnp.bfloat16)
        return x

    return jax.shard_map(local_program, mesh=mesh, in_specs=in_specs, out_specs=tok_spec, check_vma=False)
```

```python
import functools

import jax
import jax.numpy as jnp
from jax import lax
from jax.experimental import pallas as pl
from jax.experimental.pallas import tpu as pltpu
from jax.sharding import PartitionSpec as P

NORM_EPS = 1e-5
NT = (((1,), (1,)), ((), ()))
MESH = pl.DeviceIdType.MESH
CHUNKS = 2


def rms_norm(x, norm_w):
    x_f32 = x.astype(jnp.float32)
    return (x_f32 * lax.rsqrt(jnp.mean(x_f32 * x_f32, axis=-1, keepdims=True) + NORM_EPS) * norm_w).astype(jnp.bfloat16)


def route_coeffs(normed, router_w, expert_idx):
    experts = router_w.shape[-1]
    logits = jnp.dot(normed, router_w, preferred_element_type=jnp.float32)
    hit = jnp.any(expert_idx[:, :, None] == jnp.arange(experts, dtype=jnp.int32), axis=1)
    top = jnp.max(jnp.where(hit, logits, -jnp.inf), axis=-1, keepdims=True)
    exps = jnp.where(hit, jnp.exp(jnp.where(hit, logits - top, 0.0)), 0.0)
    return exps / jnp.sum(exps, axis=-1, keepdims=True)


def ring_ids(n):
    me = lax.axis_index("ep")
    return me, lax.rem(me + 1, n), lax.rem(me + n - 1, n), lax.rem(me + n // 2, n)


def enter(peers):
    barrier = pltpu.get_barrier_semaphore()
    for peer in peers:
        pl.semaphore_signal(barrier, inc=1, device_id={"ep": peer}, device_id_type=MESH)
    pl.semaphore_wait(barrier, len(peers))


def send(src, dst, sems, i, peer):
    return pltpu.make_async_remote_copy(
        src_ref=src, dst_ref=dst, send_sem=sems.at[0, i], recv_sem=sems.at[1, i], device_id={"ep": peer}, device_id_type=MESH
    )


def share_kernel(n, h_ref, c_ref, h_all, c_all, sems):
    me, up, down, far = ring_ids(n)
    half = h_ref.shape[0] // 2
    lo, hi = pl.ds(0, half), pl.ds(half, half)
    enter((up, down, far))
    up_lo = send(h_ref.at[lo], h_all.at[me, lo], sems, 0, up)
    up_hi = send(h_ref.at[hi], h_all.at[me, hi], sems, 1, up)
    down_hi = send(h_ref.at[hi], h_all.at[me, hi], sems, 2, down)
    down_lo = send(h_ref.at[lo], h_all.at[me, lo], sems, 3, down)
    coeffs = [send(c_ref.at[peer], c_all.at[me], sems, 4 + i, peer) for i, peer in enumerate((up, down, far))]
    for copy in (up_lo, down_hi, up_hi, down_lo, *coeffs):
        copy.start()
    c_all[me] = c_ref[me]
    pass_up = send(h_all.at[down, lo], h_all.at[down, lo], sems, 7, up)
    pass_down = send(h_all.at[up, hi], h_all.at[up, hi], sems, 8, down)
    up_lo.wait_recv()
    pass_up.start()
    down_hi.wait_recv()
    pass_down.start()
    for copy in (up_hi, down_lo, pass_up, pass_down, *coeffs):
        copy.wait_recv()
    for copy in (up_lo, down_hi, up_hi, down_lo, pass_up, pass_down, *coeffs):
        copy.wait_send()


def share_tokens(n, normed, coeff_t, cid):
    tokens, dim = normed.shape
    experts = coeff_t.shape[0] // n
    return pl.pallas_call(
        functools.partial(share_kernel, n),
        in_specs=[pl.BlockSpec(memory_space=pl.ANY), pl.BlockSpec(memory_space=pltpu.VMEM)],
        out_specs=[pl.BlockSpec(memory_space=pl.ANY), pl.BlockSpec(memory_space=pltpu.VMEM)],
        out_shape=[jax.ShapeDtypeStruct((n, tokens, dim), jnp.bfloat16), jax.ShapeDtypeStruct((n, experts, tokens), jnp.float32)],
        scratch_shapes=[pltpu.SemaphoreType.DMA((2, 9))],
        compiler_params=pltpu.CompilerParams(collective_id=cid, has_side_effects=True),
        cost_estimate=pl.CostEstimate(flops=60 * 10**9, bytes_accessed=8 * tokens * dim, transcendentals=0),
    )(normed, coeff_t.reshape(n, experts, tokens))


def moe_kernel(n, x_ref, h_own, h_all, c_all, w_hbm, out_ref, acc, far_in, near_in, h_buf, w_buf, act, h_sem, w_sem, sems):
    me, up, down, far = ring_ids(n)
    pieces, _, experts, rows, dim = w_hbm.shape
    chunk = h_buf.shape[1]
    half = chunk // 2
    lo, hi = pl.ds(0, half), pl.ds(half, half)
    blocks = n * CHUNKS
    steps = blocks * experts
    fp, nc = max(1, min(pieces, 256 // rows)), min(dim, 256)

    def home(s):
        k = s % n
        return lax.rem(me + jnp.where(k == 0, n // 2, jnp.where(k == 1, n - 1, jnp.where(k == 2, 1, 0))), n)

    def token_rows(s):
        return pl.ds(pl.multiple_of((s // n) * chunk, chunk), chunk)

    def load_h(s):
        @pl.when(s % n == n - 1)
        def _():
            pltpu.make_async_copy(h_own.at[token_rows(s)], h_buf.at[s % 2], h_sem.at[s % 2]).start()

        @pl.when(s % n != n - 1)
        def _():
            pltpu.make_async_copy(h_all.at[home(s), token_rows(s)], h_buf.at[s % 2], h_sem.at[s % 2]).start()

    def wait_h(s):
        pltpu.make_async_copy(h_own.at[pl.ds(0, chunk)], h_buf.at[s % 2], h_sem.at[s % 2]).wait()

    def w_copies(t):
        e, slot = t % experts, t % 2
        return [pltpu.make_async_copy(w_hbm.at[:, m, e], w_buf.at[slot, m], w_sem.at[slot, m]) for m in range(3)]

    load_h(0)
    for copy in w_copies(0):
        copy.start()
    enter((up, down))

    def far_a(c):
        return send(acc.at[n * c, lo], far_in.at[0, c], sems, 6 * c, down)

    def far_b(c):
        return send(acc.at[n * c, hi], far_in.at[1, c], sems, 6 * c + 1, up)

    def near_down(c, r, i):
        return send(acc.at[n * c + 1, r], near_in.at[0, c, r], sems, 6 * c + 2 + i, down)

    def near_up(c, r, i):
        return send(acc.at[n * c + 2, r], near_in.at[1, c, r], sems, 6 * c + 4 + i, up)

    def step(t, carry):
        s, e, slot = t // experts, t % experts, t % 2

        @pl.when(t + 1 < steps)
        def _():
            for copy in w_copies(t + 1):
                copy.start()

        @pl.when(e == 0)
        def _():
            wait_h(s)

            @pl.when(s + 1 < blocks)
            def _():
                load_h(s + 1)

        for copy in w_copies(t):
            copy.wait()
        hs = s % 2
        coeffs = c_all[home(s), token_rows(s), :]
        lane = lax.broadcasted_iota(jnp.int32, coeffs.shape, 1)
        coeff = jnp.sum(jnp.where(lane == e, coeffs, 0.0), axis=1, keepdims=True)
        for f in range(pieces // fp):
            piece = pl.ds(f * fp, fp)
            u = lax.dot_general(h_buf[hs], w_buf[slot, 0, piece].reshape(fp * rows, dim), NT, preferred_element_type=jnp.float32)
            v = lax.dot_general(h_buf[hs], w_buf[slot, 1, piece].reshape(fp * rows, dim), NT, preferred_element_type=jnp.float32)
            act[:, pl.ds(f * fp * rows, fp * rows)] = (jax.nn.silu(u) * v).astype(jnp.bfloat16)
        for j in range(dim // nc):
            cols = pl.ds(j * nc, nc)
            o = coeff * jnp.dot(act[...], w_buf[slot, 2, :, :, cols].reshape(pieces * rows, nc), preferred_element_type=jnp.float32)
            acc[s, :, cols] = jnp.where(e == 0, 0.0, acc[s, :, cols]) + o

        @pl.when(e == experts - 1)
        def _():
            for c in range(CHUNKS):

                @pl.when(s == n * c)
                def _():
                    far_a(c).start()
                    far_b(c).start()

                @pl.when(s == n * c + 1)
                def _():
                    near_down(c, hi, 1).start()

                @pl.when(s == n * c + 2)
                def _():
                    near_up(c, lo, 0).start()
                    far_a(c).wait_recv()
                    acc[n * c + 1, lo] += far_in[0, c]
                    near_down(c, lo, 0).start()

                @pl.when(s == n * c + 3)
                def _():
                    far_b(c).wait_recv()
                    acc[n * c + 2, hi] += far_in[1, c]
                    near_up(c, hi, 1).start()

        return carry

    lax.fori_loop(0, steps, step, 0)

    for c in range(CHUNKS):
        for i, r in ((1, hi), (0, lo)) if c == 0 else ((0, lo), (1, hi)):
            near_down(c, r, i).wait_recv()
            near_up(c, r, i).wait_recv()
            tok = pl.ds(c * chunk + i * half, half)
            mixed = acc[n * c + 3, r] + near_in[0, c, r] + near_in[1, c, r]
            out_ref[tok, :] = (x_ref[tok, :].astype(jnp.float32) + mixed).astype(jnp.bfloat16)
    for c in range(CHUNKS):
        far_a(c).wait_send()
        far_b(c).wait_send()
        for i, r in ((0, lo), (1, hi)):
            near_down(c, r, i).wait_send()
            near_up(c, r, i).wait_send()


def moe_layer(n, x, normed, h_all, c_all, w, cid):
    tokens, dim = x.shape
    pieces, _, experts, rows, _ = w.shape
    chunk = tokens // CHUNKS
    half = chunk // 2
    any_spec, vmem_spec = pl.BlockSpec(memory_space=pl.ANY), pl.BlockSpec(memory_space=pltpu.VMEM)
    return pl.pallas_call(
        functools.partial(moe_kernel, n),
        in_specs=[vmem_spec, any_spec, any_spec, vmem_spec, any_spec],
        out_specs=vmem_spec,
        out_shape=jax.ShapeDtypeStruct((tokens, dim), jnp.bfloat16),
        scratch_shapes=[
            pltpu.VMEM((n * CHUNKS, chunk, dim), jnp.float32),
            pltpu.VMEM((2, CHUNKS, half, dim), jnp.float32),
            pltpu.VMEM((2, CHUNKS, chunk, dim), jnp.float32),
            pltpu.VMEM((2, chunk, dim), jnp.bfloat16),
            pltpu.VMEM((2, 3, pieces, rows, dim), jnp.bfloat16),
            pltpu.VMEM((chunk, pieces * rows), jnp.bfloat16),
            pltpu.SemaphoreType.DMA((2,)),
            pltpu.SemaphoreType.DMA((2, 3)),
            pltpu.SemaphoreType.DMA((2, 6 * CHUNKS)),
        ],
        compiler_params=pltpu.CompilerParams(collective_id=cid, has_side_effects=True, vmem_limit_bytes=62 << 20),
        cost_estimate=pl.CostEstimate(
            flops=6 * n * tokens * experts * pieces * rows * dim, bytes_accessed=w.size * 2 * n * CHUNKS, transcendentals=0
        ),
    )(x, normed, h_all, c_all, w)


def solution(mesh):
    n = mesh.shape["ep"]
    tok_spec = P(("rep", "ep", "fsdp"), None)
    idx_spec = P(None, ("rep", "ep", "fsdp"), None)
    in_specs = (tok_spec, P(None, None), P(None, None, None), P(None, "ep", None, "fsdp"), P(None, "ep", None, "fsdp"), P(None, "ep", "fsdp", None), idx_spec)

    def local_program(x, norm_w, router_w, w_gate, w_up, w_down, expert_idx):
        layers = w_gate.shape[0]
        packed = [jnp.stack([w_gate[l].transpose(0, 2, 1), w_up[l].transpose(0, 2, 1), w_down[l]], axis=0) for l in range(layers)]
        gathered = [lax.all_gather(packed[l], "fsdp", axis=0) for l in range(layers)]
        for l in range(layers):
            normed = rms_norm(x, norm_w[l])
            coeff = route_coeffs(normed, router_w[l], expert_idx[l])
            h_all, c_all = share_tokens(n, normed, coeff.T, 2 * l)
            x = moe_layer(n, x, normed, h_all, c_all.transpose(0, 2, 1), gathered[l], 2 * l + 1)
        return x

    return jax.shard_map(local_program, mesh=mesh, in_specs=in_specs, out_specs=tok_spec, check_vma=False)
```

```python
import functools

import jax
import jax.numpy as jnp
from jax import lax
from jax.experimental import pallas as pl
from jax.experimental.pallas import tpu as pltpu
from jax.sharding import PartitionSpec as P

NORM_EPS = 1e-5
NT = (((1,), (1,)), ((), ()))
MESH = pl.DeviceIdType.MESH
CHUNKS = 2


def rms_norm(x, norm_w):
    x_f32 = x.astype(jnp.float32)
    return (x_f32 * lax.rsqrt(jnp.mean(x_f32 * x_f32, axis=-1, keepdims=True) + NORM_EPS) * norm_w).astype(jnp.bfloat16)


def route_coeffs(normed, router_w, expert_idx):
    experts = router_w.shape[-1]
    logits = jnp.dot(normed, router_w, preferred_element_type=jnp.float32)
    hit = jnp.any(expert_idx[:, :, None] == jnp.arange(experts, dtype=jnp.int32), axis=1)
    top = jnp.max(jnp.where(hit, logits, -jnp.inf), axis=-1, keepdims=True)
    exps = jnp.where(hit, jnp.exp(jnp.where(hit, logits - top, 0.0)), 0.0)
    return exps / jnp.sum(exps, axis=-1, keepdims=True)


def ring_ids(n):
    me = lax.axis_index("ep")
    return me, lax.rem(me + 1, n), lax.rem(me + n - 1, n), lax.rem(me + n // 2, n)


def enter(peers):
    barrier = pltpu.get_barrier_semaphore()
    for peer in peers:
        pl.semaphore_signal(barrier, inc=1, device_id={"ep": peer}, device_id_type=MESH)
    pl.semaphore_wait(barrier, len(peers))


def send(src, dst, sems, i, peer):
    return pltpu.make_async_remote_copy(
        src_ref=src, dst_ref=dst, send_sem=sems.at[0, i], recv_sem=sems.at[1, i], device_id={"ep": peer}, device_id_type=MESH
    )


def share_kernel(n, h_ref, c_ref, h_all, c_all, sems):
    me, up, down, far = ring_ids(n)
    half = h_ref.shape[0] // 2
    lo, hi = pl.ds(0, half), pl.ds(half, half)
    enter((up, down, far))
    up_lo = send(h_ref.at[lo], h_all.at[me, lo], sems, 0, up)
    up_hi = send(h_ref.at[hi], h_all.at[me, hi], sems, 1, up)
    down_hi = send(h_ref.at[hi], h_all.at[me, hi], sems, 2, down)
    down_lo = send(h_ref.at[lo], h_all.at[me, lo], sems, 3, down)
    coeffs = [send(c_ref.at[peer], c_all.at[me], sems, 4 + i, peer) for i, peer in enumerate((up, down, far))]
    for copy in (up_lo, down_hi, up_hi, down_lo, *coeffs):
        copy.start()
    c_all[me] = c_ref[me]
    pass_up = send(h_all.at[down, lo], h_all.at[down, lo], sems, 7, up)
    pass_down = send(h_all.at[up, hi], h_all.at[up, hi], sems, 8, down)
    up_lo.wait_recv()
    pass_up.start()
    down_hi.wait_recv()
    pass_down.start()
    for copy in (up_hi, down_lo, pass_up, pass_down, *coeffs):
        copy.wait_recv()
    for copy in (up_lo, down_hi, up_hi, down_lo, pass_up, pass_down, *coeffs):
        copy.wait_send()


def share_tokens(n, normed, coeff_t, cid):
    tokens, dim = normed.shape
    experts = coeff_t.shape[0] // n
    return pl.pallas_call(
        functools.partial(share_kernel, n),
        in_specs=[pl.BlockSpec(memory_space=pl.ANY), pl.BlockSpec(memory_space=pltpu.VMEM)],
        out_specs=[pl.BlockSpec(memory_space=pl.ANY), pl.BlockSpec(memory_space=pltpu.VMEM)],
        out_shape=[jax.ShapeDtypeStruct((n, tokens, dim), jnp.bfloat16), jax.ShapeDtypeStruct((n, experts, tokens), jnp.float32)],
        scratch_shapes=[pltpu.SemaphoreType.DMA((2, 9))],
        compiler_params=pltpu.CompilerParams(collective_id=cid, has_side_effects=True),
        cost_estimate=pl.CostEstimate(flops=60 * 10**9, bytes_accessed=8 * tokens * dim, transcendentals=0),
    )(normed, coeff_t.reshape(n, experts, tokens))


def add_expert(h_ref, w_ref, coeff, act, acc_ref, first):
    _, pieces, rows, dim = w_ref.shape
    fp, nc = max(1, min(pieces, 256 // rows)), min(dim, 256)
    for f in range(pieces // fp):
        piece = pl.ds(f * fp, fp)
        u = lax.dot_general(h_ref[...], w_ref[0, piece].reshape(fp * rows, dim), NT, preferred_element_type=jnp.float32)
        v = lax.dot_general(h_ref[...], w_ref[1, piece].reshape(fp * rows, dim), NT, preferred_element_type=jnp.float32)
        act[:, pl.ds(f * fp * rows, fp * rows)] = (jax.nn.silu(u) * v).astype(jnp.bfloat16)
    for j in range(dim // nc):
        cols = pl.ds(j * nc, nc)
        o = coeff * jnp.dot(act[...], w_ref[2, :, :, cols].reshape(pieces * rows, nc), preferred_element_type=jnp.float32)
        acc_ref[:, cols] = jnp.where(first, 0.0, acc_ref[:, cols]) + o


def moe_kernel(n, x_ref, h_own, h_all, c_all, w_hbm, out_ref, acc, far_in, near_in, h_buf, w_buf, act, h_sem, w_sem, sems):
    me, up, down, far = ring_ids(n)
    pieces, _, experts, rows, dim = w_hbm.shape
    chunk = h_buf.shape[1]
    half = chunk // 2
    lo, hi = pl.ds(0, half), pl.ds(half, half)
    blocks = n * CHUNKS
    steps = blocks * experts

    def home(s):
        k = s % n
        return lax.rem(me + jnp.where(k == 0, n // 2, jnp.where(k == 1, n - 1, jnp.where(k == 2, 1, 0))), n)

    def token_rows(s):
        return pl.ds(pl.multiple_of((s // n) * chunk, chunk), chunk)

    def load_h(s):
        @pl.when(s % n == n - 1)
        def _():
            pltpu.make_async_copy(h_own.at[token_rows(s)], h_buf.at[s % 2], h_sem.at[s % 2]).start()

        @pl.when(s % n != n - 1)
        def _():
            pltpu.make_async_copy(h_all.at[home(s), token_rows(s)], h_buf.at[s % 2], h_sem.at[s % 2]).start()

    def wait_h(s):
        pltpu.make_async_copy(h_own.at[pl.ds(0, chunk)], h_buf.at[s % 2], h_sem.at[s % 2]).wait()

    def w_copies(t):
        e, slot = t % experts, t % 2
        return [pltpu.make_async_copy(w_hbm.at[:, m, e], w_buf.at[slot, m], w_sem.at[slot, m]) for m in range(3)]

    load_h(0)
    for copy in w_copies(0):
        copy.start()
    enter((up, down))

    def far_a(c):
        return send(acc.at[n * c, lo], far_in.at[0, c], sems, 6 * c, down)

    def far_b(c):
        return send(acc.at[n * c, hi], far_in.at[1, c], sems, 6 * c + 1, up)

    def near_down(c, r, i):
        return send(acc.at[n * c + 1, r], near_in.at[0, c, r], sems, 6 * c + 2 + i, down)

    def near_up(c, r, i):
        return send(acc.at[n * c + 2, r], near_in.at[1, c, r], sems, 6 * c + 4 + i, up)

    def step(t, carry):
        s, e, slot = t // experts, t % experts, t % 2

        @pl.when(t + 1 < steps)
        def _():
            for copy in w_copies(t + 1):
                copy.start()

        @pl.when(e == 0)
        def _():
            wait_h(s)

            @pl.when(s + 1 < blocks)
            def _():
                load_h(s + 1)

        for copy in w_copies(t):
            copy.wait()
        hs = s % 2
        coeffs = c_all[home(s), token_rows(s), :]
        lane = lax.broadcasted_iota(jnp.int32, coeffs.shape, 1)
        coeff = jnp.sum(jnp.where(lane == e, coeffs, 0.0), axis=1, keepdims=True)
        add_expert(h_buf.at[hs], w_buf.at[slot], coeff, act, acc.at[s], e == 0)

        @pl.when(e == experts - 1)
        def _():
            for c in range(CHUNKS):

                @pl.when(s == n * c)
                def _():
                    far_a(c).start()
                    far_b(c).start()

                @pl.when(s == n * c + 1)
                def _():
                    near_down(c, hi, 1).start()

                @pl.when(s == n * c + 2)
                def _():
                    near_up(c, lo, 0).start()
                    far_a(c).wait_recv()
                    acc[n * c + 1, lo] += far_in[0, c]
                    near_down(c, lo, 0).start()

                @pl.when(s == n * c + 3)
                def _():
                    far_b(c).wait_recv()
                    acc[n * c + 2, hi] += far_in[1, c]
                    near_up(c, hi, 1).start()

        return carry

    lax.fori_loop(0, steps, step, 0)

    for c in range(CHUNKS):
        for i, r in ((1, hi), (0, lo)) if c == 0 else ((0, lo), (1, hi)):
            near_down(c, r, i).wait_recv()
            near_up(c, r, i).wait_recv()
            tok = pl.ds(c * chunk + i * half, half)
            mixed = acc[n * c + 3, r] + near_in[0, c, r] + near_in[1, c, r]
            out_ref[tok, :] = (x_ref[tok, :].astype(jnp.float32) + mixed).astype(jnp.bfloat16)
    for c in range(CHUNKS):
        far_a(c).wait_send()
        far_b(c).wait_send()
        for i, r in ((0, lo), (1, hi)):
            near_down(c, r, i).wait_send()
            near_up(c, r, i).wait_send()


def moe_layer(n, x, normed, h_all, c_all, w, cid):
    tokens, dim = x.shape
    pieces, _, experts, rows, _ = w.shape
    chunk = tokens // CHUNKS
    half = chunk // 2
    any_spec, vmem_spec = pl.BlockSpec(memory_space=pl.ANY), pl.BlockSpec(memory_space=pltpu.VMEM)
    return pl.pallas_call(
        functools.partial(moe_kernel, n),
        in_specs=[vmem_spec, any_spec, any_spec, vmem_spec, any_spec],
        out_specs=vmem_spec,
        out_shape=jax.ShapeDtypeStruct((tokens, dim), jnp.bfloat16),
        scratch_shapes=[
            pltpu.VMEM((n * CHUNKS, chunk, dim), jnp.float32),
            pltpu.VMEM((2, CHUNKS, half, dim), jnp.float32),
            pltpu.VMEM((2, CHUNKS, chunk, dim), jnp.float32),
            pltpu.VMEM((2, chunk, dim), jnp.bfloat16),
            pltpu.VMEM((2, 3, pieces, rows, dim), jnp.bfloat16),
            pltpu.VMEM((chunk, pieces * rows), jnp.bfloat16),
            pltpu.SemaphoreType.DMA((2,)),
            pltpu.SemaphoreType.DMA((2, 3)),
            pltpu.SemaphoreType.DMA((2, 6 * CHUNKS)),
        ],
        compiler_params=pltpu.CompilerParams(collective_id=cid, has_side_effects=True, vmem_limit_bytes=62 << 20),
        cost_estimate=pl.CostEstimate(
            flops=6 * n * tokens * experts * pieces * rows * dim, bytes_accessed=w.size * 2 * n * CHUNKS, transcendentals=0
        ),
    )(x, normed, h_all, c_all, w)


def pair_peer():
    me = lax.axis_index("ep")
    return me, me + 1 - 2 * (me % 2)


def pair_share_kernel(n, h_ref, c_ref, h_par, c_par, sems):
    me, peer = pair_peer()
    enter((peer,))
    copies = (
        send(h_ref, h_par, sems, 0, peer),
        send(c_ref.at[peer], c_par.at[0], sems, 1, peer),
        send(c_ref.at[n - 1 - peer], c_par.at[1], sems, 2, peer),
    )
    for copy in copies:
        copy.start()
    for copy in copies:
        copy.wait()


def pair_share(n, normed, coeff_t, cid):
    tokens, dim = normed.shape
    experts = coeff_t.shape[0] // n
    return pl.pallas_call(
        functools.partial(pair_share_kernel, n),
        in_specs=[pl.BlockSpec(memory_space=pl.ANY), pl.BlockSpec(memory_space=pltpu.VMEM)],
        out_specs=[pl.BlockSpec(memory_space=pl.ANY), pl.BlockSpec(memory_space=pltpu.VMEM)],
        out_shape=[jax.ShapeDtypeStruct((tokens, dim), jnp.bfloat16), jax.ShapeDtypeStruct((2, experts, tokens), jnp.float32)],
        scratch_shapes=[pltpu.SemaphoreType.DMA((2, 3))],
        compiler_params=pltpu.CompilerParams(collective_id=cid, has_side_effects=True),
        cost_estimate=pl.CostEstimate(flops=40 * 10**9, bytes_accessed=8 * tokens * dim, transcendentals=0),
    )(normed, coeff_t.reshape(n, experts, tokens))


def pair_kernel(x_ref, h_own, h_par, c_own, c_par, wa_hbm, wb_hbm, out_ref, acc, near_in, h_buf, w_buf, act, h_sem, w_sem, sems):
    me, peer = pair_peer()
    pieces, _, experts, rows, dim = wa_hbm.shape
    chunk = h_buf.shape[1]
    blocks, both = 2 * CHUNKS, 2 * experts
    steps = blocks * both

    def token_rows(s):
        return pl.ds(pl.multiple_of((s % CHUNKS) * chunk, chunk), chunk)

    def load_h(s):
        @pl.when(s < CHUNKS)
        def _():
            pltpu.make_async_copy(h_par.at[token_rows(s)], h_buf.at[s % 2], h_sem.at[s % 2]).start()

        @pl.when(s >= CHUNKS)
        def _():
            pltpu.make_async_copy(h_own.at[token_rows(s)], h_buf.at[s % 2], h_sem.at[s % 2]).start()

    def w_copies(w_hbm, t):
        e, slot = t % experts, t % 2
        return [pltpu.make_async_copy(w_hbm.at[:, m, e], w_buf.at[slot, m], w_sem.at[slot, m]) for m in range(3)]

    def load_w(t):
        @pl.when(t % both < experts)
        def _():
            for copy in w_copies(wa_hbm, t):
                copy.start()

        @pl.when(t % both >= experts)
        def _():
            for copy in w_copies(wb_hbm, t):
                copy.start()

    def sums(c):
        return send(acc.at[c], near_in.at[c], sems, c, peer)

    load_h(0)
    load_w(0)
    enter((peer,))

    def step(t, carry):
        s, e, slot = t // both, t % both, t % 2

        @pl.when(t + 1 < steps)
        def _():
            load_w(t + 1)

        @pl.when(e == 0)
        def _():
            pltpu.make_async_copy(h_own.at[pl.ds(0, chunk)], h_buf.at[s % 2], h_sem.at[s % 2]).wait()

            @pl.when(s + 1 < blocks)
            def _():
                load_h(s + 1)

        for copy in w_copies(wa_hbm, t):
            copy.wait()
        coeffs = jnp.where(s < CHUNKS, c_par[token_rows(s), :], c_own[token_rows(s), :])
        lane = lax.broadcasted_iota(jnp.int32, coeffs.shape, 1)
        coeff = jnp.sum(jnp.where(lane == e, coeffs, 0.0), axis=1, keepdims=True)
        add_expert(h_buf.at[s % 2], w_buf.at[slot], coeff, act, acc.at[s], e == 0)

        @pl.when(e == both - 1)
        def _():
            for c in range(CHUNKS):

                @pl.when(s == c)
                def _():
                    sums(c).start()

        return carry

    lax.fori_loop(0, steps, step, 0)
    for c in range(CHUNKS):
        sums(c).wait_recv()
        tok = pl.ds(c * chunk, chunk)
        mixed = acc[CHUNKS + c] + near_in[c]
        out_ref[tok, :] = (x_ref[tok, :].astype(jnp.float32) + mixed).astype(jnp.bfloat16)
    for c in range(CHUNKS):
        sums(c).wait_send()


def pair_layer(x, normed, h_par, c_own, c_par, wa, wb, cid):
    tokens, dim = x.shape
    pieces, _, experts, rows, _ = wa.shape
    chunk = tokens // CHUNKS
    any_spec, vmem_spec = pl.BlockSpec(memory_space=pl.ANY), pl.BlockSpec(memory_space=pltpu.VMEM)
    return pl.pallas_call(
        pair_kernel,
        in_specs=[vmem_spec, any_spec, any_spec, vmem_spec, vmem_spec, any_spec, any_spec],
        out_specs=vmem_spec,
        out_shape=jax.ShapeDtypeStruct((tokens, dim), jnp.bfloat16),
        scratch_shapes=[
            pltpu.VMEM((2 * CHUNKS, chunk, dim), jnp.float32),
            pltpu.VMEM((CHUNKS, chunk, dim), jnp.float32),
            pltpu.VMEM((2, chunk, dim), jnp.bfloat16),
            pltpu.VMEM((2, 3, pieces, rows, dim), jnp.bfloat16),
            pltpu.VMEM((chunk, pieces * rows), jnp.bfloat16),
            pltpu.SemaphoreType.DMA((2,)),
            pltpu.SemaphoreType.DMA((2, 3)),
            pltpu.SemaphoreType.DMA((2, CHUNKS)),
        ],
        compiler_params=pltpu.CompilerParams(collective_id=cid, has_side_effects=True, vmem_limit_bytes=62 << 20),
        cost_estimate=pl.CostEstimate(
            flops=24 * tokens * experts * pieces * rows * dim, bytes_accessed=wa.size * 8 * CHUNKS, transcendentals=0
        ),
    )(x, normed, h_par, c_own, c_par, wa, wb)


def solution(mesh):
    n = mesh.shape["ep"]
    tok_spec = P(("rep", "ep", "fsdp"), None)
    idx_spec = P(None, ("rep", "ep", "fsdp"), None)
    in_specs = (tok_spec, P(None, None), P(None, None, None), P(None, "ep", None, "fsdp"), P(None, "ep", None, "fsdp"), P(None, "ep", "fsdp", None), idx_spec)

    def local_program(x, norm_w, router_w, w_gate, w_up, w_down, expert_idx):
        layers = w_gate.shape[0]
        packed = [jnp.stack([w_gate[l].transpose(0, 2, 1), w_up[l].transpose(0, 2, 1), w_down[l]], axis=0) for l in range(layers)]
        last, me = layers - 1, lax.axis_index("ep")
        mirrored = lax.ppermute(packed[last], "ep", [(i, n - 1 - i) for i in range(n)])
        gathered = [lax.all_gather(packed[l], "fsdp", axis=0) for l in range(layers)]
        for l in range(layers):
            normed = rms_norm(x, norm_w[l])
            coeff = route_coeffs(normed, router_w[l], expert_idx[l])
            if l < last:
                h_all, c_all = share_tokens(n, normed, coeff.T, 2 * l)
                if l == 0:
                    h_all, mirrored = lax.optimization_barrier((h_all, mirrored))
                    gathered_mirror = lax.all_gather(mirrored, "fsdp", axis=0)
                x = moe_layer(n, x, normed, h_all, c_all.transpose(0, 2, 1), gathered[l], 2 * l + 1)
            else:
                experts = coeff.shape[1] // n
                h_par, c_par = pair_share(n, normed, coeff.T, 2 * l)
                c_own = [lax.dynamic_slice_in_dim(coeff, row * experts, experts, axis=1) for row in (me, n - 1 - me)]
                c_par = c_par.reshape(2 * experts, -1).T
                x = pair_layer(x, normed, h_par, jnp.concatenate(c_own, axis=1), c_par, gathered[l], gathered_mirror, 2 * l + 1)
        return x

    return jax.shard_map(local_program, mesh=mesh, in_specs=in_specs, out_specs=tok_spec, check_vma=False)
```

```python
import functools

import jax
import jax.numpy as jnp
from jax import lax
from jax.experimental import pallas as pl
from jax.experimental.pallas import tpu as pltpu
from jax.sharding import PartitionSpec as P

NORM_EPS = 1e-5
NT = (((1,), (1,)), ((), ()))
MESH = pl.DeviceIdType.MESH
CHUNKS = 2


def rms_norm(x, norm_w):
    x_f32 = x.astype(jnp.float32)
    return (x_f32 * lax.rsqrt(jnp.mean(x_f32 * x_f32, axis=-1, keepdims=True) + NORM_EPS) * norm_w).astype(jnp.bfloat16)


def route_coeffs(normed, router_w, expert_idx):
    experts = router_w.shape[-1]
    logits = jnp.dot(normed, router_w, preferred_element_type=jnp.float32)
    hit = jnp.any(expert_idx[:, :, None] == jnp.arange(experts, dtype=jnp.int32), axis=1)
    top = jnp.max(jnp.where(hit, logits, -jnp.inf), axis=-1, keepdims=True)
    exps = jnp.where(hit, jnp.exp(jnp.where(hit, logits - top, 0.0)), 0.0)
    return exps / jnp.sum(exps, axis=-1, keepdims=True)


def ring_ids(n):
    me = lax.axis_index("ep")
    return me, lax.rem(me + 1, n), lax.rem(me + n - 1, n), lax.rem(me + n // 2, n)


def enter(peers):
    barrier = pltpu.get_barrier_semaphore()
    for peer in peers:
        pl.semaphore_signal(barrier, inc=1, device_id={"ep": peer}, device_id_type=MESH)
    pl.semaphore_wait(barrier, len(peers))


def send(src, dst, sems, i, peer):
    return pltpu.make_async_remote_copy(
        src_ref=src, dst_ref=dst, send_sem=sems.at[0, i], recv_sem=sems.at[1, i], device_id={"ep": peer}, device_id_type=MESH
    )


def share_kernel(n, h_ref, c_ref, h_all, c_all, sems):
    me, up, down, far = ring_ids(n)
    half = h_ref.shape[0] // 2
    lo, hi = pl.ds(0, half), pl.ds(half, half)
    enter((up, down, far))
    up_lo = send(h_ref.at[lo], h_all.at[me, lo], sems, 0, up)
    up_hi = send(h_ref.at[hi], h_all.at[me, hi], sems, 1, up)
    down_hi = send(h_ref.at[hi], h_all.at[me, hi], sems, 2, down)
    down_lo = send(h_ref.at[lo], h_all.at[me, lo], sems, 3, down)
    coeffs = [send(c_ref.at[peer], c_all.at[me], sems, 4 + i, peer) for i, peer in enumerate((up, down, far))]
    for copy in (up_lo, down_hi, up_hi, down_lo, *coeffs):
        copy.start()
    c_all[me] = c_ref[me]
    pass_up = send(h_all.at[down, lo], h_all.at[down, lo], sems, 7, up)
    pass_down = send(h_all.at[up, hi], h_all.at[up, hi], sems, 8, down)
    up_lo.wait_recv()
    pass_up.start()
    down_hi.wait_recv()
    pass_down.start()
    for copy in (up_hi, down_lo, pass_up, pass_down, *coeffs):
        copy.wait_recv()
    for copy in (up_lo, down_hi, up_hi, down_lo, pass_up, pass_down, *coeffs):
        copy.wait_send()


def share_tokens(n, normed, coeff_t, cid):
    tokens, dim = normed.shape
    experts = coeff_t.shape[0] // n
    return pl.pallas_call(
        functools.partial(share_kernel, n),
        in_specs=[pl.BlockSpec(memory_space=pl.ANY), pl.BlockSpec(memory_space=pltpu.VMEM)],
        out_specs=[pl.BlockSpec(memory_space=pl.ANY), pl.BlockSpec(memory_space=pltpu.VMEM)],
        out_shape=[jax.ShapeDtypeStruct((n, tokens, dim), jnp.bfloat16), jax.ShapeDtypeStruct((n, experts, tokens), jnp.float32)],
        scratch_shapes=[pltpu.SemaphoreType.DMA((2, 9))],
        compiler_params=pltpu.CompilerParams(collective_id=cid, has_side_effects=True),
        cost_estimate=pl.CostEstimate(flops=60 * 10**9, bytes_accessed=8 * tokens * dim, transcendentals=0),
    )(normed, coeff_t.reshape(n, experts, tokens))


def add_expert(h_ref, get, dims, coeff, act, acc_ref, first):
    pieces, rows, dim = dims
    fp, nc = max(1, min(pieces, 256 // rows)), min(dim, 256)
    every = slice(None)
    for f in range(pieces // fp):
        piece = pl.ds(f * fp, fp)
        u = lax.dot_general(h_ref[...], get(0, piece, every).reshape(fp * rows, dim), NT, preferred_element_type=jnp.float32)
        v = lax.dot_general(h_ref[...], get(1, piece, every).reshape(fp * rows, dim), NT, preferred_element_type=jnp.float32)
        act[:, pl.ds(f * fp * rows, fp * rows)] = (jax.nn.silu(u) * v).astype(jnp.bfloat16)
    for j in range(dim // nc):
        cols = pl.ds(j * nc, nc)
        o = coeff * jnp.dot(act[...], get(2, every, cols).reshape(pieces * rows, nc), preferred_element_type=jnp.float32)
        acc_ref[:, cols] = o if first is True else jnp.where(first, 0.0, acc_ref[:, cols]) + o


def pick(coeffs, e):
    lane = lax.broadcasted_iota(jnp.int32, coeffs.shape, 1)
    return jnp.sum(jnp.where(lane == e, coeffs, 0.0), axis=1, keepdims=True)


def block_kernel(h_ref, c_ref, w_ref, out_ref, act):
    e = pl.program_id(0)
    pieces, _, _, rows, dim = w_ref.shape
    add_expert(h_ref, lambda m, p, cols: w_ref[p, m, 0, :, cols], (pieces, rows, dim), pick(c_ref[...], e), act, out_ref, e == 0)


def block_ffn(h, coeff, w):
    tokens, dim = h.shape
    pieces, _, experts, rows, _ = w.shape
    return pl.pallas_call(
        block_kernel,
        grid=(experts,),
        in_specs=[
            pl.BlockSpec((tokens, dim), lambda e: (0, 0)),
            pl.BlockSpec((tokens, experts), lambda e: (0, 0)),
            pl.BlockSpec((pieces, 3, 1, rows, dim), lambda e: (0, 0, e, 0, 0)),
        ],
        out_specs=pl.BlockSpec((tokens, dim), lambda e: (0, 0)),
        out_shape=jax.ShapeDtypeStruct((tokens, dim), jnp.float32),
        scratch_shapes=[pltpu.VMEM((tokens, pieces * rows), jnp.bfloat16)],
        compiler_params=pltpu.CompilerParams(dimension_semantics=("arbitrary",), vmem_limit_bytes=60 << 20),
        cost_estimate=pl.CostEstimate(
            flops=6 * tokens * experts * pieces * rows * dim, bytes_accessed=w.size * 2, transcendentals=0
        ),
    )(h, coeff, w)


def moe_kernel(n, x_ref, h_own, h_all, c_all, w_hbm, far_hbm, out_ref, acc, far_out, far_in, near_in, h_buf, w_buf, act, h_sem, w_sem, far_sem, sems):
    me, up, down, _ = ring_ids(n)
    m1 = n - 1
    pieces, _, experts, rows, dim = w_hbm.shape
    chunk = h_buf.shape[1]
    half = chunk // 2
    lo, hi = pl.ds(0, half), pl.ds(half, half)
    blocks = m1 * CHUNKS
    steps = blocks * experts

    def home(s):
        k = s % m1
        return lax.rem(me + jnp.where(k == 0, n - 1, jnp.where(k == 1, 1, 0)), n)

    def token_rows(s):
        return pl.ds(pl.multiple_of((s // m1) * chunk, chunk), chunk)

    def load_h(s):
        @pl.when(s % m1 == m1 - 1)
        def _():
            pltpu.make_async_copy(h_own.at[token_rows(s)], h_buf.at[s % 2], h_sem.at[s % 2]).start()

        @pl.when(s % m1 != m1 - 1)
        def _():
            pltpu.make_async_copy(h_all.at[home(s), token_rows(s)], h_buf.at[s % 2], h_sem.at[s % 2]).start()

    def wait_h(s):
        pltpu.make_async_copy(h_own.at[pl.ds(0, chunk)], h_buf.at[s % 2], h_sem.at[s % 2]).wait()

    def w_copies(t):
        e, slot = t % experts, t % 2
        return [pltpu.make_async_copy(w_hbm.at[:, m, e], w_buf.at[slot, m], w_sem.at[slot, m]) for m in range(3)]

    far_loads = [pltpu.make_async_copy(far_hbm.at[pl.ds(c * chunk, chunk)], far_out.at[c], far_sem.at[c]) for c in range(CHUNKS)]
    for copy in far_loads:
        copy.start()
    load_h(0)
    for copy in w_copies(0):
        copy.start()
    enter((up, down))

    def far_a(c):
        return send(far_out.at[c, lo], far_in.at[0, c], sems, 6 * c, down)

    def far_b(c):
        return send(far_out.at[c, hi], far_in.at[1, c], sems, 6 * c + 1, up)

    def near_down(c, r, i):
        return send(acc.at[m1 * c, r], near_in.at[0, c, r], sems, 6 * c + 2 + i, down)

    def near_up(c, r, i):
        return send(acc.at[m1 * c + 1, r], near_in.at[1, c, r], sems, 6 * c + 4 + i, up)

    for c in range(CHUNKS):
        far_loads[c].wait()
        far_a(c).start()
        far_b(c).start()

    def step(t, carry):
        s, e, slot = t // experts, t % experts, t % 2

        @pl.when(t + 1 < steps)
        def _():
            for copy in w_copies(t + 1):
                copy.start()

        @pl.when(e == 0)
        def _():
            wait_h(s)

            @pl.when(s + 1 < blocks)
            def _():
                load_h(s + 1)

        for copy in w_copies(t):
            copy.wait()
        hs = s % 2
        add_expert(
            h_buf.at[hs], lambda m, p, cols: w_buf[slot, m, p, :, cols], (pieces, rows, dim),
            pick(c_all[home(s), token_rows(s), :], e), act, acc.at[s], e == 0,
        )

        @pl.when(e == experts - 1)
        def _():
            for c in range(CHUNKS):

                @pl.when(s == m1 * c)
                def _():
                    near_down(c, hi, 1).start()

                @pl.when(s == m1 * c + 1)
                def _():
                    near_up(c, lo, 0).start()
                    far_a(c).wait_recv()
                    acc[m1 * c, lo] += far_in[0, c]
                    near_down(c, lo, 0).start()

                @pl.when(s == m1 * c + 2)
                def _():
                    far_b(c).wait_recv()
                    acc[m1 * c + 1, hi] += far_in[1, c]
                    near_up(c, hi, 1).start()

        return carry

    lax.fori_loop(0, steps, step, 0)

    for c in range(CHUNKS):
        for i, r in ((1, hi), (0, lo)) if c == 0 else ((0, lo), (1, hi)):
            near_down(c, r, i).wait_recv()
            near_up(c, r, i).wait_recv()
            tok = pl.ds(c * chunk + i * half, half)
            mixed = acc[m1 * c + 2, r] + near_in[0, c, r] + near_in[1, c, r]
            out_ref[tok, :] = (x_ref[tok, :].astype(jnp.float32) + mixed).astype(jnp.bfloat16)
    for c in range(CHUNKS):
        far_a(c).wait_send()
        far_b(c).wait_send()
        for i, r in ((0, lo), (1, hi)):
            near_down(c, r, i).wait_send()
            near_up(c, r, i).wait_send()


def moe_layer(n, x, normed, h_all, c_all, w, far_part, cid):
    tokens, dim = x.shape
    pieces, _, experts, rows, _ = w.shape
    chunk = tokens // CHUNKS
    half = chunk // 2
    any_spec, vmem_spec = pl.BlockSpec(memory_space=pl.ANY), pl.BlockSpec(memory_space=pltpu.VMEM)
    return pl.pallas_call(
        functools.partial(moe_kernel, n),
        in_specs=[vmem_spec, any_spec, any_spec, vmem_spec, any_spec, any_spec],
        out_specs=vmem_spec,
        out_shape=jax.ShapeDtypeStruct((tokens, dim), jnp.bfloat16),
        scratch_shapes=[
            pltpu.VMEM(((n - 1) * CHUNKS, chunk, dim), jnp.float32),
            pltpu.VMEM((CHUNKS, chunk, dim), jnp.float32),
            pltpu.VMEM((2, CHUNKS, half, dim), jnp.float32),
            pltpu.VMEM((2, CHUNKS, chunk, dim), jnp.float32),
            pltpu.VMEM((2, chunk, dim), jnp.bfloat16),
            pltpu.VMEM((2, 3, pieces, rows, dim), jnp.bfloat16),
            pltpu.VMEM((chunk, pieces * rows), jnp.bfloat16),
            pltpu.SemaphoreType.DMA((2,)),
            pltpu.SemaphoreType.DMA((2, 3)),
            pltpu.SemaphoreType.DMA((CHUNKS,)),
            pltpu.SemaphoreType.DMA((2, 6 * CHUNKS)),
        ],
        compiler_params=pltpu.CompilerParams(collective_id=cid, has_side_effects=True, vmem_limit_bytes=62 << 20),
        cost_estimate=pl.CostEstimate(
            flops=6 * (n - 1) * tokens * experts * pieces * rows * dim, bytes_accessed=w.size * 2 * n * CHUNKS, transcendentals=0
        ),
    )(x, normed, h_all, c_all, w, far_part)


def pair_peer():
    me = lax.axis_index("ep")
    return me, me + 1 - 2 * (me % 2)


def expert_loop(seq, sources, h_buf, w_buf, act, acc, load_h, wait_h, coeffs, h_sem, w_sem, w_hbm, done, fresh):
    pieces, _, experts, rows, dim = w_hbm[0].shape
    count = len(seq)

    def at(q, j):
        value = seq[0][j]
        for i in range(1, count):
            value = jnp.where(q >= i, seq[i][j], value)
        return value

    def w_copies(src, t):
        e, slot = t % experts, t % 2
        return [pltpu.make_async_copy(src.at[:, m, e], w_buf.at[slot, m], w_sem.at[slot, m]) for m in range(3)]

    def load_w(t):
        if sources == 1:
            for copy in w_copies(w_hbm[0], t):
                copy.start()
            return
        for i in range(2):

            @pl.when(at(t // experts, 1) == i)
            def _():
                for copy in w_copies(w_hbm[i], t):
                    copy.start()

    load_w(0)
    load_h(0)

    def step(t, carry):
        q, e, slot = t // experts, t % experts, t % 2

        @pl.when(t + 1 < count * experts)
        def _():
            load_w(t + 1)

        @pl.when(e == 0)
        def _():
            wait_h(q)

            @pl.when(q + 1 < count)
            def _():
                load_h(q + 1)

        for copy in w_copies(w_hbm[0], t):
            copy.wait()
        add_expert(
            h_buf.at[q % 2], lambda m, p, cols: w_buf[slot, m, p, :, cols], (pieces, rows, dim),
            pick(coeffs(q), at(q, 1) * experts + e), act, acc.at[at(q, 0)], jnp.logical_and(e == 0, fresh(q)),
        )

        @pl.when(e == experts - 1)
        def _():
            done(q)

        return carry

    lax.fori_loop(0, count * experts, step, 0)


def pair_first_kernel(h_own, c_own, c_send, wa_hbm, h_par, c_par, part_hbm, acc, c_now, h_buf, w_buf, act, h_sem, w_sem, part_sem, sems):
    me, peer = pair_peer()
    chunk = h_buf.shape[1]
    rows_of = [pl.ds(c * chunk, chunk) for c in range(CHUNKS)]
    enter((peer,))
    swaps = []
    for c in range(CHUNKS):
        swaps.append(send(c_send.at[rows_of[c]], c_par.at[rows_of[c]], sems, 2 * c, peer))
        swaps.append(send(h_own.at[rows_of[c]], h_par.at[rows_of[c]], sems, 2 * c + 1, peer))
    for copy in swaps:
        copy.start()

    def load_h(q):
        for i in range(CHUNKS):

            @pl.when(q == i)
            def _():
                pltpu.make_async_copy(h_own.at[rows_of[i]], h_buf.at[q % 2], h_sem.at[q % 2]).start()

    def wait_h(q):
        @pl.when(q == CHUNKS)
        def _():
            swaps[0].wait_recv()
            swaps[1].wait_recv()
            pltpu.make_async_copy(h_par.at[rows_of[0]], h_buf.at[q % 2], h_sem.at[q % 2]).start()
            c_now[...] = c_par[rows_of[0], :]

        for i in range(CHUNKS):

            @pl.when(q == i)
            def _():
                c_now[...] = c_own[rows_of[i], :]

        pltpu.make_async_copy(h_own.at[rows_of[0]], h_buf.at[q % 2], h_sem.at[q % 2]).wait()

    def coeffs(q):
        return c_now[...]

    def part(i):
        return pltpu.make_async_copy(acc.at[i], part_hbm.at[i], part_sem.at[i])

    def done(q):
        for i in range(CHUNKS + 1):

            @pl.when(q == i)
            def _():
                part(i).start()

    seq = [(i, 0) for i in range(CHUNKS + 1)]
    expert_loop(seq, 1, h_buf, w_buf, act, acc, load_h, wait_h, coeffs, h_sem, w_sem, (wa_hbm,), done, lambda q: q >= 0)
    for copy in swaps[2:]:
        copy.wait_recv()
    for copy in swaps:
        copy.wait_send()
    for i in range(CHUNKS + 1):
        part(i).wait()


def pair_second_kernel(x_ref, h_own, h_par, c_own, c_par, part_hbm, wa_hbm, wb_hbm, out_ref, acc, near_in, h_buf, w_buf, act, h_sem, w_sem, part_sem, sems):
    me, peer = pair_peer()
    chunk = h_buf.shape[1]
    parts = [pltpu.make_async_copy(part_hbm.at[i], acc.at[i], part_sem.at[i]) for i in (2, 0, 1)]
    for copy in parts:
        copy.start()
    enter((peer,))
    seq = [(2, 1), (3, 0), (3, 1), (0, 1), (1, 1)]
    tokens = [(h_par, c_par, 0), (h_par, c_par, 1), (h_par, c_par, 1), (h_own, c_own, 0), (h_own, c_own, 1)]

    def sums(c):
        return send(acc.at[CHUNKS + c], near_in.at[c], sems, c, peer)

    def load_h(q):
        for i, (h_ref, _, c) in enumerate(tokens):

            @pl.when(q == i)
            def _():
                pltpu.make_async_copy(h_ref.at[pl.ds(c * chunk, chunk)], h_buf.at[q % 2], h_sem.at[q % 2]).start()

    def wait_h(q):
        pltpu.make_async_copy(h_own.at[pl.ds(0, chunk)], h_buf.at[q % 2], h_sem.at[q % 2]).wait()
        for copy, i in zip(parts, (0, 3, 4)):

            @pl.when(q == i)
            def _():
                copy.wait()

    def coeffs(q):
        second = jnp.logical_or(q == 4, jnp.logical_or(q == 1, q == 2))
        rows = pl.ds(pl.multiple_of(jnp.where(second, chunk, 0), chunk), chunk)
        return jnp.where(q < 3, c_par[rows, :], c_own[rows, :])

    def done(q):
        for i, c in ((0, 0), (2, 1)):

            @pl.when(q == i)
            def _():
                sums(c).start()

    expert_loop(seq, 2, h_buf, w_buf, act, acc, load_h, wait_h, coeffs, h_sem, w_sem, (wa_hbm, wb_hbm), done, lambda q: q == 1)
    for c in range(CHUNKS):
        sums(c).wait_recv()
        tok = pl.ds(c * chunk, chunk)
        out_ref[tok, :] = (x_ref[tok, :].astype(jnp.float32) + (acc[c] + near_in[c])).astype(jnp.bfloat16)
    for c in range(CHUNKS):
        sums(c).wait_send()


def pair_layer(x, normed, c_own, c_send, wa, other_row, cid):
    tokens, dim = x.shape
    pieces, _, experts, rows, _ = wa.shape
    chunk = tokens // CHUNKS
    any_spec, vmem_spec = pl.BlockSpec(memory_space=pl.ANY), pl.BlockSpec(memory_space=pltpu.VMEM)
    bufs = [
        pltpu.VMEM((2, chunk, dim), jnp.bfloat16),
        pltpu.VMEM((2, 3, pieces, rows, dim), jnp.bfloat16),
        pltpu.VMEM((chunk, pieces * rows), jnp.bfloat16),
        pltpu.SemaphoreType.DMA((2,)),
        pltpu.SemaphoreType.DMA((2, 3)),
        pltpu.SemaphoreType.DMA((CHUNKS + 1,)),
    ]
    work = 6 * chunk * experts * pieces * rows * dim
    h_par, c_par, part = pl.pallas_call(
        pair_first_kernel,
        in_specs=[any_spec, vmem_spec, vmem_spec, any_spec],
        out_specs=[any_spec, vmem_spec, any_spec],
        out_shape=[
            jax.ShapeDtypeStruct(normed.shape, jnp.bfloat16),
            jax.ShapeDtypeStruct(c_own.shape, jnp.float32),
            jax.ShapeDtypeStruct((CHUNKS + 1, chunk, dim), jnp.float32),
        ],
        scratch_shapes=[
            pltpu.VMEM((CHUNKS + 1, chunk, dim), jnp.float32), pltpu.VMEM((chunk, c_own.shape[1]), jnp.float32), *bufs,
            pltpu.SemaphoreType.DMA((2, 2 * CHUNKS)),
        ],
        compiler_params=pltpu.CompilerParams(collective_id=cid, has_side_effects=True, vmem_limit_bytes=62 << 20),
        cost_estimate=pl.CostEstimate(flops=3 * work, bytes_accessed=wa.size * 6, transcendentals=0),
    )(normed, c_own, c_send, wa)
    return pl.pallas_call(
        pair_second_kernel,
        in_specs=[vmem_spec, any_spec, any_spec, vmem_spec, vmem_spec, any_spec, any_spec, any_spec],
        out_specs=vmem_spec,
        out_shape=jax.ShapeDtypeStruct((tokens, dim), jnp.bfloat16),
        scratch_shapes=[
            pltpu.VMEM((2 * CHUNKS, chunk, dim), jnp.float32),
            pltpu.VMEM((CHUNKS, chunk, dim), jnp.float32),
            *bufs,
            pltpu.SemaphoreType.DMA((2, CHUNKS)),
        ],
        compiler_params=pltpu.CompilerParams(collective_id=cid + 1, has_side_effects=True, vmem_limit_bytes=62 << 20),
        cost_estimate=pl.CostEstimate(flops=5 * work, bytes_accessed=wa.size * 10, transcendentals=0),
    )(x, normed, h_par, c_own, c_par, part, wa, other_row)


def solution(mesh):
    n = mesh.shape["ep"]
    tok_spec = P(("rep", "ep", "fsdp"), None)
    idx_spec = P(None, ("rep", "ep", "fsdp"), None)
    in_specs = (tok_spec, P(None, None), P(None, None, None), P(None, "ep", None, "fsdp"), P(None, "ep", None, "fsdp"), P(None, "ep", "fsdp", None), idx_spec)

    def local_program(x, norm_w, router_w, w_gate, w_up, w_down, expert_idx):
        layers = w_gate.shape[0]
        packed = [jnp.stack([w_gate[l].transpose(0, 2, 1), w_up[l].transpose(0, 2, 1), w_down[l]], axis=0) for l in range(layers)]
        last, me = layers - 1, lax.axis_index("ep")
        gathered = [lax.all_gather(packed[l], "fsdp", axis=0) for l in range(layers)]
        gathered_mirror = None
        for l in range(layers):
            normed = rms_norm(x, norm_w[l])
            coeff = route_coeffs(normed, router_w[l], expert_idx[l])
            experts = coeff.shape[1] // n
            if l < last:
                h_all, c_all = share_tokens(n, normed, coeff.T, 2 * l)
                c_all = c_all.transpose(0, 2, 1)
                far = lax.rem(me + n // 2, n)
                if l == 0:
                    h_all, to_send = lax.optimization_barrier((h_all, packed[last]))
                    mirrored = lax.ppermute(to_send, "ep", [(i, n - 1 - i) for i in range(n)])
                far_part = block_ffn(
                    lax.dynamic_index_in_dim(h_all, far, keepdims=False), lax.dynamic_index_in_dim(c_all, far, keepdims=False), gathered[l]
                )
                if l == 0:
                    far_part, mirrored = lax.optimization_barrier((far_part, mirrored))
                    gathered_mirror = lax.all_gather(mirrored, "fsdp", axis=0)
                x = moe_layer(n, x, normed, h_all, c_all, gathered[l], far_part, 2 * l + 1)
            else:
                peer = me + 1 - 2 * (me % 2)

                def rows_for(who):
                    cols = [lax.dynamic_slice_in_dim(coeff, row * experts, experts, axis=1) for row in (who, n - 1 - who)]
                    return jnp.pad(jnp.concatenate(cols, axis=1), ((0, 0), (0, max(0, 128 - 2 * experts))))

                x = pair_layer(x, normed, rows_for(me), rows_for(peer), gathered[l], gathered_mirror, 2 * l)
        return x

    return jax.shard_map(local_program, mesh=mesh, in_specs=in_specs, out_specs=tok_spec, check_vma=False)
```
